32 devices in a mesh: site: 2 (over x), row: 4 (over z), col: 4 (over y, core).
Axes of the slice: x: 2, y: 2, z: 4, core: 2. Of those that a mesh axis runs over, the one named last changes fastest.
Arguments:
- pair_array: bfloat16 [128, 64, 128], P(('site', 'row'), 'col'), parts along dimension 0, may hold values from -6 to 6
- in_gain: float32 [128], replicated, may hold values from 0.25 to 1.75
- left_weight: bfloat16 [256, 128], P('site'), parts along dimension 0, may hold values from -0.5 to 0.5
- right_weight: bfloat16 [256, 128], P('site'), parts along dimension 0, may hold values from -0.5 to 0.5
- mid_gain: float32 [128], replicated, may hold values from 0.25 to 1.75
- out_weight: bfloat16 [256, 128], P('site'), parts along dimension 0, may hold values from -0.5 to 0.5
- out_gate: bfloat16 [256, 128], P('site'), parts along dimension 0, may hold values from -0.5 to 0.5
Outputs:
- triangle_out: bfloat16 [128, 64, 128], P(('site', 'row'), 'col'), parts along dimension 0
The draws below stay inside these ranges and needn't reach their ends.
There are 2 independent parts, one for each index of `site`. The reference program is written for one: setup_inputs(seed, part) draws one part's arguments, and reference() takes and returns one part's arrays. A program takes and returns all parts, laid end to end along the dimension named above; an argument that names none is the same for every part. Nothing has to cross between parts.
All inputs are finite; a program needn't handle non-finite values.
Results may differ from the reference program's by a relative error of at most 0.012.
Values may be sent and summed in bfloat16 or wider, within the bound.
A program may use at most 64 MiB of HBM per device.

```python
import jax
import jax.numpy as jnp
from jax import lax

RESIDUES = 64
PAIR_WIDTH = 128
MIX_WIDTH = 128


def block_levels(rng, extent, cuts, low, high):
    loudness = 1.0
    for dim, blocks in cuts:
        steps = jax.random.uniform(jax.random.fold_in(jax.random.fold_in(rng, 6), dim), (blocks,), jnp.float32, low / len(cuts), high / len(cuts))
        loudness = loudness * jnp.repeat(jnp.exp(steps), extent[dim] // blocks).reshape((-1,) + (1,) * (len(extent) - 1 - dim))
    return loudness


def scatter_about(key, extent, spread, reach, pieces=(), held_as=jnp.bfloat16):
    drawn = jax.random.normal(key, extent, jnp.float32) * spread
    if len(pieces) > 0:
        drawn = block_levels(key, extent, pieces, -0.22, 0.18) * drawn
    return jnp.clip(drawn, min=-reach, max=reach).astype(held_as)


def setup_inputs(seed: int = 0, part: int = 0) -> dict:
    keys = jax.random.split(jax.random.key(seed), 8)
    part_keys = jax.random.split(jax.random.fold_in(keys[7], part), 8)
    return {
        "pair_array": scatter_about(part_keys[0], (RESIDUES, RESIDUES, PAIR_WIDTH), 1.0, 6.0, ((0, 4), (1, 4))),
        "in_gain": jnp.clip(1.0 + 0.15 * jax.random.normal(keys[1], (PAIR_WIDTH,), jnp.float32), 0.25, 1.75),
        "left_weight": scatter_about(part_keys[2], (PAIR_WIDTH, MIX_WIDTH), PAIR_WIDTH ** -0.5, 0.5),
        "right_weight": scatter_about(part_keys[3], (PAIR_WIDTH, MIX_WIDTH), PAIR_WIDTH ** -0.5, 0.5),
        "mid_gain": jnp.clip(1.0 + 0.15 * jax.random.normal(keys[4], (MIX_WIDTH,), jnp.float32), 0.25, 1.75),
        "out_weight": scatter_about(part_keys[5], (MIX_WIDTH, PAIR_WIDTH), MIX_WIDTH ** -0.5, 0.5),
        "out_gate": scatter_about(part_keys[6], (PAIR_WIDTH, PAIR_WIDTH), PAIR_WIDTH ** -0.5, 0.5),
    }


def norm_channels(values, channel_gain):
    centred = values - lax.optimization_barrier(jnp.mean(values, axis=-1, keepdims=True))
    return centred * lax.rsqrt(lax.optimization_barrier(jnp.mean(centred * centred, axis=-1, keepdims=True)) + 1e-05) * channel_gain

def both_factors(pair_in, in_gain, left_weight, right_weight):
    ready = norm_channels(pair_in.astype(jnp.float32), in_gain).astype(jnp.bfloat16)
    ready = lax.optimization_barrier(ready)
    left = jnp.einsum('ijc,cd->ijd', ready.astype(jnp.float32), left_weight.astype(jnp.float32))
    right = jnp.einsum('ijc,cd->ijd', ready.astype(jnp.float32), right_weight.astype(jnp.float32))
    return (ready, left.astype(jnp.bfloat16), right.astype(jnp.bfloat16))

def finish_pair(mixed, ready, mid_gain, out_weight, out_gate):
    scaled = norm_channels(mixed.astype(jnp.float32), mid_gain).astype(jnp.bfloat16)
    scaled = lax.optimization_barrier(scaled)
    gate = jax.nn.sigmoid(jnp.einsum('ijc,cd->ijd', ready.astype(jnp.float32), out_gate.astype(jnp.float32)))
    return (jnp.einsum('ijd,dc->ijc', scaled.astype(jnp.float32), out_weight.astype(jnp.float32)) * gate).astype(jnp.bfloat16)

def reference(pair_array, in_gain, left_weight, right_weight, mid_gain, out_weight, out_gate):
    ready, left, right = both_factors(pair_array, in_gain, left_weight, right_weight)
    left, right = lax.optimization_barrier((left, right))

    def one_channel(pair_of):
        return (jnp.dot(pair_of[0].T, pair_of[1], preferred_element_type=jnp.float32) * RESIDUES ** (-0.5)).astype(jnp.bfloat16)
    mixed = jnp.moveaxis(lax.map(one_channel, (jnp.moveaxis(left, -1, 0), jnp.moveaxis(right, -1, 0))), 0, -1)
    mixed = lax.optimization_barrier(mixed)
    return finish_pair(mixed, ready, mid_gain, out_weight, out_gate)
```

```python
import functools

import jax
import jax.numpy as jnp
from jax import lax
from jax.experimental import pallas as pl
from jax.experimental.pallas import tpu as pltpu
from jax.sharding import PartitionSpec as P


def norm_channels(values, channel_gain):
    centred = values - jnp.mean(values, axis=-1, keepdims=True)
    return (
        centred
        * lax.rsqrt(jnp.mean(centred * centred, axis=-1, keepdims=True) + 1e-05)
        * channel_gain
    )


def both_factors(pair_in, in_gain, left_weight, right_weight):
    ready = norm_channels(pair_in.astype(jnp.float32), in_gain).astype(jnp.bfloat16)
    ready = lax.optimization_barrier(ready)
    left = jnp.einsum("ijc,cd->ijd", ready, left_weight, preferred_element_type=jnp.float32)
    right = jnp.einsum("ijc,cd->ijd", ready, right_weight, preferred_element_type=jnp.float32)
    return (ready, left.astype(jnp.bfloat16), right.astype(jnp.bfloat16))


def finish_pair(mixed, ready, mid_gain, out_weight, out_gate):
    scaled = norm_channels(mixed.astype(jnp.float32), mid_gain).astype(jnp.bfloat16)
    scaled = lax.optimization_barrier(scaled)
    gate = jax.nn.sigmoid(
        jnp.einsum("ijc,cd->ijd", ready, out_gate, preferred_element_type=jnp.float32)
    )
    return (
        jnp.einsum("ijd,dc->ijc", scaled, out_weight, preferred_element_type=jnp.float32) * gate
    ).astype(jnp.bfloat16)


def body(pair_array, in_gain, left_weight, right_weight, mid_gain, out_weight, out_gate):
    ready, left, right = both_factors(pair_array, in_gain, left_weight, right_weight)
    count = pair_array.shape[0] * lax.axis_size("row")
    left_lines, right_lines = (
        lax.all_to_all(left, "row", split_axis=2, concat_axis=0, tiled=True),
        lax.all_to_all(right, "row", split_axis=2, concat_axis=0, tiled=True),
    )
    strip = jnp.einsum(
        "kid,kjd->ijd",
        lax.all_gather(left_lines, "col", axis=1, tiled=True),
        right_lines,
        preferred_element_type=jnp.float32,
    )
    strip = (strip * count ** (-0.5)).astype(jnp.bfloat16)
    mixed = lax.all_to_all(strip, "row", split_axis=0, concat_axis=2, tiled=True)
    return finish_pair(mixed, ready, mid_gain, out_weight, out_gate)


MESH = pl.DeviceIdType.MESH


def flip(index, mask, count):
    flipped, bit = 0, 1
    while bit < count:
        digit = (index // bit) % 2
        flipped = flipped + bit * ((1 - digit) if mask & bit else digit)
        bit *= 2
    return flipped


def fused(
    count, halves, scale,
    pair_hbm, in_gain_hbm, left_hbm, right_hbm, mid_gain_hbm, out_hbm, gate_hbm,
    result,
    pair, in_gain, left_w, right_w, mid_gain, out_w, gate_w,
    ready, left_send, left_got, right, wide, part_send, part_got, own, gate,
    load_sem, lsend_sem, lgot_sem, psend_sem, pgot_sem,
):
    row, col = lax.axis_index("row"), lax.axis_index("col")
    lines, width = pair.shape[0], pair.shape[1]
    piece = width // halves
    barrier = pltpu.get_barrier_semaphore()
    for mask in range(1, count):
        pl.semaphore_signal(
            barrier, inc=1, device_id={"col": flip(col, mask, count)}, device_id_type=MESH
        )
        pl.semaphore_signal(
            barrier, inc=1, device_id={"row": flip(row, mask, count)}, device_id_type=MESH
        )
    loads = [
        pltpu.make_async_copy(src, dst, load_sem.at[n])
        for n, (src, dst) in enumerate(
            [
                (pair_hbm, pair), (in_gain_hbm, in_gain), (left_hbm, left_w),
                (right_hbm, right_w), (mid_gain_hbm, mid_gain), (out_hbm, out_w),
                (gate_hbm, gate_w),
            ]
        )
    ]
    for load in loads:
        load.start()
    loads[0].wait()
    loads[1].wait()
    channels = pair.shape[2]
    values = pair[...].reshape(lines * width, channels).astype(jnp.float32)
    ready[...] = norm_channels(values, in_gain[...]).astype(jnp.bfloat16)
    loads[2].wait()
    left = jnp.dot(ready[...], left_w[...], preferred_element_type=jnp.float32)
    depth = left.shape[-1]
    left = left.reshape(lines, halves, piece, depth)
    for half in range(halves):
        left_send[half] = left[:, half].reshape(lines * piece, depth).astype(jnp.bfloat16)
    loads[3].wait()
    right[...] = (
        jnp.dot(ready[...], right_w[...], preferred_element_type=jnp.float32)
        .astype(jnp.bfloat16).astype(jnp.float32)
    )

    pl.semaphore_wait(barrier, 2 * (count - 1))

    def left_copy(mask, half):
        return pltpu.make_async_remote_copy(
            src_ref=left_send.at[half],
            dst_ref=left_got.at[mask - 1, half],
            send_sem=lsend_sem.at[mask - 1, half],
            recv_sem=lgot_sem.at[mask - 1, half],
            device_id={"col": flip(col, mask, count)},
            device_id_type=MESH,
        )

    for half in range(halves):
        for mask in range(1, count):
            left_copy(mask, half).start()

    def part_copy(mask, half):
        return pltpu.make_async_remote_copy(
            src_ref=part_send.at[mask, half],
            dst_ref=part_got.at[row, half],
            send_sem=psend_sem.at[mask, half],
            recv_sem=pgot_sem.at[row, half],
            device_id={"row": flip(col, mask, count)},
            device_id_type=MESH,
        )

    def products(mask, half):
        source = left_send.at[half] if mask == 0 else left_got.at[mask - 1, half]
        wide[...] = source[...].astype(jnp.float32)

        def total():
            sums = [None] * piece
            for k in range(lines):
                across = right[k * width : (k + 1) * width, :]
                for i in range(piece):
                    at = k * piece + i
                    term = wide[at : at + 1, :] * across
                    sums[i] = term if k == 0 else sums[i] + term
            return sums

        target = flip(col, mask, count)
        sums = total()

        @pl.when(target == row)
        def _():
            for i in range(piece):
                own[half, i * width : (i + 1) * width, :] = sums[i]

        @pl.when(target != row)
        def _():
            for i in range(piece):
                part_send[mask, half, i * width : (i + 1) * width, :] = sums[i].astype(jnp.bfloat16)
            part_copy(mask, half).start()

    for mask in range(count):
        for half in range(halves):
            if mask >= 2:
                break
            if mask:
                left_copy(mask, half).wait_recv()
            products(mask, half)
    loads[6].wait()
    gate[...] = jax.nn.sigmoid(
        jnp.dot(ready[...], gate_w[...], preferred_element_type=jnp.float32)
    )
    for half in range(halves):
        for mask in range(2, count):
            left_copy(mask, half).wait_recv()
            products(mask, half)
    loads[4].wait()
    loads[5].wait()
    for half in range(halves):
        mixed = own[half]
        for mask in range(1, count):
            peer = flip(row, mask, count)
            pltpu.make_async_remote_copy(
                src_ref=part_send.at[0, half],
                dst_ref=part_got.at[peer, half],
                send_sem=psend_sem.at[0, half],
                recv_sem=pgot_sem.at[peer, half],
                device_id={"row": peer},
                device_id_type=MESH,
            ).wait_recv()
            mixed = mixed + part_got[peer, half].astype(jnp.float32)
        mixed = (mixed * scale).astype(jnp.bfloat16).astype(jnp.float32)
        scaled = norm_channels(mixed, mid_gain[...]).astype(jnp.bfloat16)
        rows = piece * width
        made = jnp.dot(scaled, out_w[...], preferred_element_type=jnp.float32)
        made = made * gate[half * rows : (half + 1) * rows, :]
        result[half * piece : (half + 1) * piece] = made.astype(jnp.bfloat16).reshape(
            piece, width, channels
        )
    for half in range(halves):
        for mask in range(1, count):
            left_copy(mask, half).wait_send()
        for mask in range(count):

            @pl.when(flip(col, mask, count) != row)
            def _(mask=mask, half=half):
                part_copy(mask, half).wait_send()


def fused_body(pair_array, in_gain, left_weight, right_weight, mid_gain, out_weight, out_gate):
    count = lax.axis_size("row")
    lines, width, channels = pair_array.shape
    depth = left_weight.shape[1]
    halves = max(width // 8, 1)
    piece = width // halves
    scale = (lines * count) ** (-0.5)
    low, high = jnp.bfloat16, jnp.float32
    return pl.pallas_call(
        functools.partial(fused, count, halves, scale),
        out_shape=jax.ShapeDtypeStruct(pair_array.shape, low),
        in_specs=[pl.BlockSpec(memory_space=pl.ANY)] * 7,
        out_specs=pl.BlockSpec(memory_space=pltpu.VMEM),
        scratch_shapes=[
            pltpu.VMEM(pair_array.shape, low),
            pltpu.VMEM((1, channels), high),
            pltpu.VMEM(left_weight.shape, low),
            pltpu.VMEM(right_weight.shape, low),
            pltpu.VMEM((1, depth), high),
            pltpu.VMEM(out_weight.shape, low),
            pltpu.VMEM(out_gate.shape, low),
            pltpu.VMEM((lines * width, channels), low),
            pltpu.VMEM((halves, lines * piece, depth), low),
            pltpu.VMEM((count - 1, halves, lines * piece, depth), low),
            pltpu.VMEM((lines * width, depth), high),
            pltpu.VMEM((lines * piece, depth), high),
            pltpu.VMEM((count, halves, piece * width, depth), low),
            pltpu.VMEM((count, halves, piece * width, depth), low),
            pltpu.VMEM((halves, piece * width, depth), high),
            pltpu.VMEM((lines * width, channels), high),
            pltpu.SemaphoreType.DMA((7,)),
            pltpu.SemaphoreType.DMA((count - 1, halves)),
            pltpu.SemaphoreType.DMA((count - 1, halves)),
            pltpu.SemaphoreType.DMA((count, halves)),
            pltpu.SemaphoreType.DMA((count, halves)),
        ],
        compiler_params=pltpu.CompilerParams(collective_id=0, has_side_effects=True),
        name="triangle",
    )(
        pair_array, in_gain.reshape(1, -1), left_weight, right_weight,
        mid_gain.reshape(1, -1), out_weight, out_gate,
    )


def pick(pair_array, *rest):
    rows, cols = lax.axis_size("row"), lax.axis_size("col")
    square = rows == cols and rows & (rows - 1) == 0
    square = square and pair_array.shape[0] == pair_array.shape[1]
    return (fused_body if square else body)(pair_array, *rest)


def solution(mesh):
    return jax.shard_map(
        pick,
        mesh=mesh,
        in_specs=(
            P(("site", "row"), "col", None),
            P(),
            P("site", None),
            P("site", None),
            P(),
            P("site", None),
            P("site", None),
        ),
        out_specs=P(("site", "row"), "col", None),
        check_vma=False,
    )
```

```python
import functools

import jax
import jax.numpy as jnp
from jax import lax
from jax.experimental import pallas as pl
from jax.experimental.pallas import tpu as pltpu
from jax.sharding import PartitionSpec as P


def norm_channels(values, channel_gain):
    centred = values - jnp.mean(values, axis=-1, keepdims=True)
    return (
        centred
        * lax.rsqrt(jnp.mean(centred * centred, axis=-1, keepdims=True) + 1e-05)
        * channel_gain
    )


def both_factors(pair_in, in_gain, left_weight, right_weight):
    ready = norm_channels(pair_in.astype(jnp.float32), in_gain).astype(jnp.bfloat16)
    ready = lax.optimization_barrier(ready)
    left = jnp.einsum("ijc,cd->ijd", ready, left_weight, preferred_element_type=jnp.float32)
    right = jnp.einsum("ijc,cd->ijd", ready, right_weight, preferred_element_type=jnp.float32)
    return (ready, left.astype(jnp.bfloat16), right.astype(jnp.bfloat16))


def finish_pair(mixed, ready, mid_gain, out_weight, out_gate):
    scaled = norm_channels(mixed.astype(jnp.float32), mid_gain).astype(jnp.bfloat16)
    scaled = lax.optimization_barrier(scaled)
    gate = jax.nn.sigmoid(
        jnp.einsum("ijc,cd->ijd", ready, out_gate, preferred_element_type=jnp.float32)
    )
    return (
        jnp.einsum("ijd,dc->ijc", scaled, out_weight, preferred_element_type=jnp.float32) * gate
    ).astype(jnp.bfloat16)


def body(pair_array, in_gain, left_weight, right_weight, mid_gain, out_weight, out_gate):
    ready, left, right = both_factors(pair_array, in_gain, left_weight, right_weight)
    count = pair_array.shape[0] * lax.axis_size("row")
    left_lines, right_lines = (
        lax.all_to_all(left, "row", split_axis=2, concat_axis=0, tiled=True),
        lax.all_to_all(right, "row", split_axis=2, concat_axis=0, tiled=True),
    )
    strip = jnp.einsum(
        "kid,kjd->ijd",
        lax.all_gather(left_lines, "col", axis=1, tiled=True),
        right_lines,
        preferred_element_type=jnp.float32,
    )
    strip = (strip * count ** (-0.5)).astype(jnp.bfloat16)
    mixed = lax.all_to_all(strip, "row", split_axis=0, concat_axis=2, tiled=True)
    return finish_pair(mixed, ready, mid_gain, out_weight, out_gate)


MESH = pl.DeviceIdType.MESH


def flip(index, mask, count):
    flipped, bit = 0, 1
    while bit < count:
        digit = (index // bit) % 2
        flipped = flipped + bit * ((1 - digit) if mask & bit else digit)
        bit *= 2
    return flipped


def fused(
    count, scale,
    pair_hbm, in_gain_hbm, left_hbm, right_hbm, mid_gain_hbm, out_hbm, gate_hbm,
    result,
    pair, in_gain, left_w, right_w, mid_gain, out_w, gate_w,
    ready, left_send, left_got, right_send, right_got, right, wide, part_send, part_got, own, gate,
    load_sem, lsend_sem, lgot_sem, rsend_sem, rgot_sem, psend_sem, pgot_sem,
):
    row, col = lax.axis_index("row"), lax.axis_index("col")
    half = col % 2
    twin = flip(col, 1, count)
    lines, width = pair.shape[0], pair.shape[1]
    piece = width // 2
    barrier = pltpu.get_barrier_semaphore()
    for mask in range(1, count):
        there = flip(row, mask, count)
        for device in ({"col": flip(col, mask, count)}, {"row": there}, {"row": there, "col": twin}):
            pl.semaphore_signal(barrier, inc=1, device_id=device, device_id_type=MESH)
    loads = [
        pltpu.make_async_copy(src, dst, load_sem.at[n])
        for n, (src, dst) in enumerate(
            [
                (pair_hbm, pair), (in_gain_hbm, in_gain), (left_hbm, left_w),
                (right_hbm, right_w), (mid_gain_hbm, mid_gain), (out_hbm, out_w),
                (gate_hbm, gate_w),
            ]
        )
    ]
    for load in loads:
        load.start()
    loads[0].wait()
    loads[1].wait()
    channels = pair.shape[2]
    values = pair[...].reshape(lines * width, channels).astype(jnp.float32)
    ready[...] = norm_channels(values, in_gain[...]).astype(jnp.bfloat16)
    loads[2].wait()
    left = jnp.dot(ready[...], left_w[...], preferred_element_type=jnp.float32)
    depth = left.shape[-1]
    left = left.reshape(lines, 2, piece, depth)
    for part in range(2):
        left_send[part] = left[:, part].reshape(lines * piece, depth).astype(jnp.bfloat16)
    loads[3].wait()
    right_send[...] = jnp.dot(
        ready[...], right_w[...], preferred_element_type=jnp.float32
    ).astype(jnp.bfloat16)

    pl.semaphore_wait(barrier, 3 * (count - 1))

    def left_copy(mask):
        return pltpu.make_async_remote_copy(
            src_ref=left_send.at[(half + mask) % 2],
            dst_ref=left_got.at[mask - 1],
            send_sem=lsend_sem.at[mask - 1],
            recv_sem=lgot_sem.at[mask - 1],
            device_id={"col": flip(col, mask, count)},
            device_id_type=MESH,
        )

    right_copy = pltpu.make_async_remote_copy(
        src_ref=right_send,
        dst_ref=right_got,
        send_sem=rsend_sem,
        recv_sem=rgot_sem,
        device_id={"col": twin},
        device_id_type=MESH,
    )
    for mask in range(2, count):
        left_copy(mask).start()
    right_copy.start()
    left_copy(1).start()

    def part_copy(mask, side):
        return pltpu.make_async_remote_copy(
            src_ref=part_send.at[mask, side],
            dst_ref=part_got.at[row, half],
            send_sem=psend_sem.at[mask, side],
            recv_sem=pgot_sem.at[row, half],
            device_id={"row": flip(col, mask, count), "col": twin if side else col},
            device_id_type=MESH,
        )

    def products(mask, side):
        sums = [None] * piece
        for k in range(lines):
            across = right[side, k * width : (k + 1) * width, :]
            for i in range(piece):
                at = k * piece + i
                term = wide[mask, at : at + 1, :] * across
                sums[i] = term if k == 0 else sums[i] + term

        def send():
            for i in range(piece):
                part_send[mask, side, i * width : (i + 1) * width, :] = sums[i].astype(jnp.bfloat16)
            part_copy(mask, side).start()

        if side:
            send()
        else:
            here = flip(col, mask, count) == row

            @pl.when(here)
            def _():
                for i in range(piece):
                    own[i * width : (i + 1) * width, :] = sums[i]

            pl.when(jnp.logical_not(here))(send)

    right[0] = right_send[...].astype(jnp.float32)
    wide[0] = left_send[half].astype(jnp.float32)
    products(0, 0)
    right_copy.wait_recv()
    right[1] = right_got[...].astype(jnp.float32)
    products(0, 1)
    for mask in range(1, count):
        left_copy(mask).wait_recv()
        wide[mask] = left_got[mask - 1].astype(jnp.float32)
        products(mask, 0)
        products(mask, 1)
        if mask == 1:
            loads[6].wait()
            gate[...] = jax.nn.sigmoid(
                jnp.dot(ready[...], gate_w[...], preferred_element_type=jnp.float32)
            )
    loads[4].wait()
    loads[5].wait()

    def arrived(peer, part):
        pltpu.make_async_remote_copy(
            src_ref=part_send.at[0, 0],
            dst_ref=part_got.at[peer, part],
            send_sem=psend_sem.at[0, 0],
            recv_sem=pgot_sem.at[peer, part],
            device_id={"row": row, "col": twin},
            device_id_type=MESH,
        ).wait_recv()
        return part_got[peer, part].astype(jnp.float32)

    rows = piece * width
    for part, mixed in ((half, own[...]), (1 - half, arrived(row, 1 - half))):
        for mask in range(1, count):
            mixed = mixed + arrived(flip(row, mask, count), part)
        mixed = (mixed * scale).astype(jnp.bfloat16).astype(jnp.float32)
        scaled = norm_channels(mixed, mid_gain[...]).astype(jnp.bfloat16)
        made = jnp.dot(scaled, out_w[...], preferred_element_type=jnp.float32)
        made = made * gate[pl.ds(pl.multiple_of(part * rows, rows), rows), :]
        result[pl.ds(part * piece, piece)] = made.astype(jnp.bfloat16).reshape(
            piece, width, channels
        )
    for mask in range(1, count):
        left_copy(mask).wait_send()
    right_copy.wait_send()
    for mask in range(count):
        part_copy(mask, 1).wait_send()

        @pl.when(flip(col, mask, count) != row)
        def _(mask=mask):
            part_copy(mask, 0).wait_send()


def fused_body(pair_array, in_gain, left_weight, right_weight, mid_gain, out_weight, out_gate):
    count = lax.axis_size("row")
    lines, width, channels = pair_array.shape
    depth = left_weight.shape[1]
    piece = width // 2
    scale = (lines * count) ** (-0.5)
    low, high = jnp.bfloat16, jnp.float32
    return pl.pallas_call(
        functools.partial(fused, count, scale),
        out_shape=jax.ShapeDtypeStruct(pair_array.shape, low),
        in_specs=[pl.BlockSpec(memory_space=pl.ANY)] * 7,
        out_specs=pl.BlockSpec(memory_space=pltpu.VMEM),
        scratch_shapes=[
            pltpu.VMEM(pair_array.shape, low),
            pltpu.VMEM((1, channels), high),
            pltpu.VMEM(left_weight.shape, low),
            pltpu.VMEM(right_weight.shape, low),
            pltpu.VMEM((1, depth), high),
            pltpu.VMEM(out_weight.shape, low),
            pltpu.VMEM(out_gate.shape, low),
            pltpu.VMEM((lines * width, channels), low),
            pltpu.VMEM((2, lines * piece, depth), low),
            pltpu.VMEM((count - 1, lines * piece, depth), low),
            pltpu.VMEM((lines * width, depth), low),
            pltpu.VMEM((lines * width, depth), low),
            pltpu.VMEM((2, lines * width, depth), high),
            pltpu.VMEM((count, lines * piece, depth), high),
            pltpu.VMEM((count, 2, piece * width, depth), low),
            pltpu.VMEM((count, 2, piece * width, depth), low),
            pltpu.VMEM((piece * width, depth), high),
            pltpu.VMEM((lines * width, channels), high),
            pltpu.SemaphoreType.DMA((7,)),
            pltpu.SemaphoreType.DMA((count - 1,)),
            pltpu.SemaphoreType.DMA((count - 1,)),
            pltpu.SemaphoreType.DMA,
            pltpu.SemaphoreType.DMA,
            pltpu.SemaphoreType.DMA((count, 2)),
            pltpu.SemaphoreType.DMA((count, 2)),
        ],
        compiler_params=pltpu.CompilerParams(collective_id=0, has_side_effects=True),
        name="triangle",
    )(
        pair_array, in_gain.reshape(1, -1), left_weight, right_weight,
        mid_gain.reshape(1, -1), out_weight, out_gate,
    )


def pick(pair_array, *rest):
    rows, cols = lax.axis_size("row"), lax.axis_size("col")
    square = rows == cols > 1 and rows & (rows - 1) == 0
    square = square and pair_array.shape[0] == pair_array.shape[1]
    square = square and pair_array.shape[1] % 16 == 0
    return (fused_body if square else body)(pair_array, *rest)


def solution(mesh):
    return jax.shard_map(
        pick,
        mesh=mesh,
        in_specs=(
            P(("site", "row"), "col", None),
            P(),
            P("site", None),
            P("site", None),
            P(),
            P("site", None),
            P("site", None),
        ),
        out_specs=P(("site", "row"), "col", None),
        check_vma=False,
    )
```

```python
import functools

import jax
import jax.numpy as jnp
from jax import lax
from jax.experimental import pallas as pl
from jax.experimental.pallas import tpu as pltpu
from jax.sharding import PartitionSpec as P


def norm_channels(values, channel_gain):
    centred = values - jnp.mean(values, axis=-1, keepdims=True)
    return (
        centred
        * lax.rsqrt(jnp.mean(centred * centred, axis=-1, keepdims=True) + 1e-05)
        * channel_gain
    )


def both_factors(pair_in, in_gain, left_weight, right_weight):
    ready = norm_channels(pair_in.astype(jnp.float32), in_gain).astype(jnp.bfloat16)
    ready = lax.optimization_barrier(ready)
    left = jnp.einsum("ijc,cd->ijd", ready, left_weight, preferred_element_type=jnp.float32)
    right = jnp.einsum("ijc,cd->ijd", ready, right_weight, preferred_element_type=jnp.float32)
    return (ready, left.astype(jnp.bfloat16), right.astype(jnp.bfloat16))


def finish_pair(mixed, ready, mid_gain, out_weight, out_gate):
    scaled = norm_channels(mixed.astype(jnp.float32), mid_gain).astype(jnp.bfloat16)
    scaled = lax.optimization_barrier(scaled)
    gate = jax.nn.sigmoid(
        jnp.einsum("ijc,cd->ijd", ready, out_gate, preferred_element_type=jnp.float32)
    )
    return (
        jnp.einsum("ijd,dc->ijc", scaled, out_weight, preferred_element_type=jnp.float32) * gate
    ).astype(jnp.bfloat16)


def body(pair_array, in_gain, left_weight, right_weight, mid_gain, out_weight, out_gate):
    ready, left, right = both_factors(pair_array, in_gain, left_weight, right_weight)
    count = pair_array.shape[0] * lax.axis_size("row")
    left_lines, right_lines = (
        lax.all_to_all(left, "row", split_axis=2, concat_axis=0, tiled=True),
        lax.all_to_all(right, "row", split_axis=2, concat_axis=0, tiled=True),
    )
    strip = jnp.einsum(
        "kid,kjd->ijd",
        lax.all_gather(left_lines, "col", axis=1, tiled=True),
        right_lines,
        preferred_element_type=jnp.float32,
    )
    strip = (strip * count ** (-0.5)).astype(jnp.bfloat16)
    mixed = lax.all_to_all(strip, "row", split_axis=0, concat_axis=2, tiled=True)
    return finish_pair(mixed, ready, mid_gain, out_weight, out_gate)


MESH = pl.DeviceIdType.MESH


def flip(index, mask, count):
    flipped, bit = 0, 1
    while bit < count:
        digit = (index // bit) % 2
        flipped = flipped + bit * ((1 - digit) if mask & bit else digit)
        bit *= 2
    return flipped


def fused(
    count, scale,
    pair_hbm, in_gain_hbm, left_hbm, right_hbm, mid_gain_hbm, out_hbm, gate_hbm,
    result,
    pair, in_gain, left_w, right_w, mid_gain, out_w, gate_w,
    ready, left_send, left_got, right_send, right_got, right, wide, part_send, part_got, own, gate,
    load_sem, lsend_sem, lgot_sem, rsend_sem, rgot_sem, psend_sem, pgot_sem,
):
    row, col = lax.axis_index("row"), lax.axis_index("col")
    half = col % 2
    twin = flip(col, 1, count)
    lines, width = pair.shape[0], pair.shape[1]
    piece = width // 2
    barrier = pltpu.get_barrier_semaphore()
    for mask in range(1, count):
        there = flip(row, mask, count)
        for device in ({"col": flip(col, mask, count)}, {"row": there}, {"row": there, "col": twin}):
            pl.semaphore_signal(barrier, inc=1, device_id=device, device_id_type=MESH)
    loads = [
        pltpu.make_async_copy(src, dst, load_sem.at[n])
        for n, (src, dst) in enumerate(
            [
                (pair_hbm, pair), (in_gain_hbm, in_gain), (left_hbm, left_w),
                (right_hbm, right_w), (mid_gain_hbm, mid_gain), (out_hbm, out_w),
                (gate_hbm, gate_w),
            ]
        )
    ]
    for load in loads:
        load.start()
    loads[0].wait()
    loads[1].wait()
    channels = pair.shape[2]
    values = pair[...].reshape(lines * width, channels).astype(jnp.float32)
    ready[...] = norm_channels(values, in_gain[...]).astype(jnp.bfloat16)
    loads[2].wait()
    left = jnp.dot(ready[...], left_w[...], preferred_element_type=jnp.float32)
    depth = left.shape[-1]
    left = left.reshape(lines, 2, piece, depth)
    for part in range(2):
        left_send[part] = left[:, part].reshape(lines * piece, depth).astype(jnp.bfloat16)
    loads[3].wait()
    right_send[...] = jnp.dot(
        ready[...], right_w[...], preferred_element_type=jnp.float32
    ).astype(jnp.bfloat16)

    pl.semaphore_wait(barrier, 3 * (count - 1))

    def left_copy(mask):
        return pltpu.make_async_remote_copy(
            src_ref=left_send.at[(half + mask) % 2],
            dst_ref=left_got.at[mask - 1],
            send_sem=lsend_sem.at[mask - 1],
            recv_sem=lgot_sem.at[mask - 1],
            device_id={"col": flip(col, mask, count)},
            device_id_type=MESH,
        )

    right_copy = pltpu.make_async_remote_copy(
        src_ref=right_send,
        dst_ref=right_got,
        send_sem=rsend_sem,
        recv_sem=rgot_sem,
        device_id={"col": twin},
        device_id_type=MESH,
    )
    for mask in range(2, count):
        left_copy(mask).start()
    right_copy.start()
    left_copy(1).start()

    def part_copy(mask, side):
        return pltpu.make_async_remote_copy(
            src_ref=part_send.at[mask, side],
            dst_ref=part_got.at[row, half],
            send_sem=psend_sem.at[mask, side],
            recv_sem=pgot_sem.at[row, half],
            device_id={"row": flip(col, mask, count), "col": twin if side else col},
            device_id_type=MESH,
        )

    def products(mask, side):
        sums = [None] * piece
        for k in range(lines):
            across = right[side, k * width : (k + 1) * width, :]
            for i in range(piece):
                at = k * piece + i
                term = wide[mask, at : at + 1, :] * across
                sums[i] = term if k == 0 else sums[i] + term

        def send():
            for i in range(piece):
                part_send[mask, side, i * width : (i + 1) * width, :] = sums[i].astype(jnp.bfloat16)
            part_copy(mask, side).start()

        if side:
            send()
        else:
            here = flip(col, mask, count) == row

            @pl.when(here)
            def _():
                for i in range(piece):
                    own[i * width : (i + 1) * width, :] = sums[i]

            pl.when(jnp.logical_not(here))(send)

    right[0] = right_send[...].astype(jnp.float32)
    wide[0] = left_send[half].astype(jnp.float32)
    products(0, 0)
    right_copy.wait_recv()
    right[1] = right_got[...].astype(jnp.float32)
    products(0, 1)
    for mask in range(1, count):
        left_copy(mask).wait_recv()
        wide[mask] = left_got[mask - 1].astype(jnp.float32)
        products(mask, 0)
        products(mask, 1)
        if mask == 1:
            loads[6].wait()
            gate[...] = jax.nn.sigmoid(
                jnp.dot(ready[...], gate_w[...], preferred_element_type=jnp.float32)
            )
    loads[4].wait()
    loads[5].wait()

    def arrived(peer, part):
        pltpu.make_async_remote_copy(
            src_ref=part_send.at[0, 0],
            dst_ref=part_got.at[peer, part],
            send_sem=psend_sem.at[0, 0],
            recv_sem=pgot_sem.at[peer, part],
            device_id={"row": row, "col": twin},
            device_id_type=MESH,
        ).wait_recv()
        return part_got[peer, part].astype(jnp.float32)

    rows = piece * width
    for part, mixed in ((half, own[...]), (1 - half, arrived(row, 1 - half))):
        for mask in range(1, count):
            mixed = mixed + arrived(flip(row, mask, count), part)
        mixed = (mixed * scale).astype(jnp.bfloat16).astype(jnp.float32)
        scaled = norm_channels(mixed, mid_gain[...]).astype(jnp.bfloat16)
        made = jnp.dot(scaled, out_w[...], preferred_element_type=jnp.float32)
        made = made * gate[pl.ds(pl.multiple_of(part * rows, rows), rows), :]
        result[pl.ds(part * piece, piece)] = made.astype(jnp.bfloat16).reshape(
            piece, width, channels
        )
    for mask in range(1, count):
        left_copy(mask).wait_send()
    right_copy.wait_send()
    for mask in range(count):
        part_copy(mask, 1).wait_send()

        @pl.when(flip(col, mask, count) != row)
        def _(mask=mask):
            part_copy(mask, 0).wait_send()


def fused_body(pair_array, in_gain, left_weight, right_weight, mid_gain, out_weight, out_gate):
    count = lax.axis_size("row")
    lines, width, channels = pair_array.shape
    depth = left_weight.shape[1]
    piece = width // 2
    scale = (lines * count) ** (-0.5)
    low, high = jnp.bfloat16, jnp.float32
    return pl.pallas_call(
        functools.partial(fused, count, scale),
        out_shape=pltpu.VMEM(pair_array.shape, low),
        in_specs=[pl.BlockSpec(memory_space=pl.ANY)] * 7,
        out_specs=pl.BlockSpec(memory_space=pltpu.VMEM),
        scratch_shapes=[
            pltpu.VMEM(pair_array.shape, low),
            pltpu.VMEM((1, channels), high),
            pltpu.VMEM(left_weight.shape, low),
            pltpu.VMEM(right_weight.shape, low),
            pltpu.VMEM((1, depth), high),
            pltpu.VMEM(out_weight.shape, low),
            pltpu.VMEM(out_gate.shape, low),
            pltpu.VMEM((lines * width, channels), low),
            pltpu.VMEM((2, lines * piece, depth), low),
            pltpu.VMEM((count - 1, lines * piece, depth), low),
            pltpu.VMEM((lines * width, depth), low),
            pltpu.VMEM((lines * width, depth), low),
            pltpu.VMEM((2, lines * width, depth), high),
            pltpu.VMEM((count, lines * piece, depth), high),
            pltpu.VMEM((count, 2, piece * width, depth), low),
            pltpu.VMEM((count, 2, piece * width, depth), low),
            pltpu.VMEM((piece * width, depth), high),
            pltpu.VMEM((lines * width, channels), high),
            pltpu.SemaphoreType.DMA((7,)),
            pltpu.SemaphoreType.DMA((count - 1,)),
            pltpu.SemaphoreType.DMA((count - 1,)),
            pltpu.SemaphoreType.DMA,
            pltpu.SemaphoreType.DMA,
            pltpu.SemaphoreType.DMA((count, 2)),
            pltpu.SemaphoreType.DMA((count, 2)),
        ],
        compiler_params=pltpu.CompilerParams(collective_id=0, has_side_effects=True),
        name="triangle",
    )(
        pair_array, in_gain.reshape(1, -1), left_weight, right_weight,
        mid_gain.reshape(1, -1), out_weight, out_gate,
    )


def pick(pair_array, *rest):
    rows, cols = lax.axis_size("row"), lax.axis_size("col")
    square = rows == cols > 1 and rows & (rows - 1) == 0
    square = square and pair_array.shape[0] == pair_array.shape[1]
    square = square and pair_array.shape[1] % 16 == 0
    return (fused_body if square else body)(pair_array, *rest)


def solution(mesh):
    return jax.shard_map(
        pick,
        mesh=mesh,
        in_specs=(
            P(("site", "row"), "col", None),
            P(),
            P("site", None),
            P("site", None),
            P(),
            P("site", None),
            P("site", None),
        ),
        out_specs=P(("site", "row"), "col", None),
        check_vma=False,
    )
```

```python
import functools

import jax
import jax.numpy as jnp
from jax import lax
from jax.experimental import pallas as pl
from jax.experimental.pallas import tpu as pltpu
from jax.sharding import PartitionSpec as P


def norm_channels(values, channel_gain):
    centred = values - jnp.mean(values, axis=-1, keepdims=True)
    return (
        centred
        * lax.rsqrt(jnp.mean(centred * centred, axis=-1, keepdims=True) + 1e-05)
        * channel_gain
    )


def both_factors(pair_in, in_gain, left_weight, right_weight):
    ready = norm_channels(pair_in.astype(jnp.float32), in_gain).astype(jnp.bfloat16)
    ready = lax.optimization_barrier(ready)
    left = jnp.einsum("ijc,cd->ijd", ready, left_weight, preferred_element_type=jnp.float32)
    right = jnp.einsum("ijc,cd->ijd", ready, right_weight, preferred_element_type=jnp.float32)
    return (ready, left.astype(jnp.bfloat16), right.astype(jnp.bfloat16))


def finish_pair(mixed, ready, mid_gain, out_weight, out_gate):
    scaled = norm_channels(mixed.astype(jnp.float32), mid_gain).astype(jnp.bfloat16)
    scaled = lax.optimization_barrier(scaled)
    gate = jax.nn.sigmoid(
        jnp.einsum("ijc,cd->ijd", ready, out_gate, preferred_element_type=jnp.float32)
    )
    return (
        jnp.einsum("ijd,dc->ijc", scaled, out_weight, preferred_element_type=jnp.float32) * gate
    ).astype(jnp.bfloat16)


def body(pair_array, in_gain, left_weight, right_weight, mid_gain, out_weight, out_gate):
    ready, left, right = both_factors(pair_array, in_gain, left_weight, right_weight)
    count = pair_array.shape[0] * lax.axis_size("row")
    left_lines, right_lines = (
        lax.all_to_all(left, "row", split_axis=2, concat_axis=0, tiled=True),
        lax.all_to_all(right, "row", split_axis=2, concat_axis=0, tiled=True),
    )
    strip = jnp.einsum(
        "kid,kjd->ijd",
        lax.all_gather(left_lines, "col", axis=1, tiled=True),
        right_lines,
        preferred_element_type=jnp.float32,
    )
    strip = (strip * count ** (-0.5)).astype(jnp.bfloat16)
    mixed = lax.all_to_all(strip, "row", split_axis=0, concat_axis=2, tiled=True)
    return finish_pair(mixed, ready, mid_gain, out_weight, out_gate)


MESH = pl.DeviceIdType.MESH


def flip(index, mask, count):
    flipped, bit = 0, 1
    while bit < count:
        digit = (index // bit) % 2
        flipped = flipped + bit * ((1 - digit) if mask & bit else digit)
        bit *= 2
    return flipped


def fused(
    count, scale,
    pair_hbm, in_gain_hbm, left_hbm, right_hbm, mid_gain_hbm, out_hbm, gate_hbm,
    result,
    pair, in_gain, left_w, right_w, mid_gain, out_w, gate_w,
    ready, left_send, left_got, right_send, right_got, right, wide, part_send, part_got, own, gate,
    load_sem, lsend_sem, lgot_sem, rsend_sem, rgot_sem, psend_sem, pgot_sem,
    near_sem, far_sem,
):
    row, col = lax.axis_index("row"), lax.axis_index("col")
    half = col % 2
    twin = flip(col, 1, count)
    lines, width = pair.shape[0], pair.shape[1]
    piece = width // 2
    barrier = pltpu.get_barrier_semaphore()
    for n in range(count // 2):
        odd = 2 * n + 1

        @pl.when(odd != col)
        def _(odd=odd):
            pl.semaphore_signal(barrier, inc=1, device_id={"col": odd}, device_id_type=MESH)

    for mask in range(1, count):
        pl.semaphore_signal(
            barrier, inc=1, device_id={"row": flip(row, mask, count), "col": col - half},
            device_id_type=MESH,
        )
    loads = [
        pltpu.make_async_copy(src, dst, load_sem.at[n])
        for n, (src, dst) in enumerate(
            [
                (pair_hbm, pair), (in_gain_hbm, in_gain), (left_hbm, left_w),
                (right_hbm, right_w), (mid_gain_hbm, mid_gain), (out_hbm, out_w),
                (gate_hbm, gate_w),
            ]
        )
    ]
    for load in loads:
        load.start()
    loads[0].wait()
    loads[1].wait()
    channels = pair.shape[2]
    values = pair[...].reshape(lines * width, channels).astype(jnp.float32)
    ready[...] = norm_channels(values, in_gain[...]).astype(jnp.bfloat16)
    loads[2].wait()
    left = jnp.dot(ready[...], left_w[...], preferred_element_type=jnp.float32)
    depth = left.shape[-1]
    left = left.reshape(lines, 2, piece, depth)
    for part in range(2):
        left_send[part] = left[:, part].reshape(lines * piece, depth).astype(jnp.bfloat16)
    loads[3].wait()
    right_send[...] = jnp.dot(
        ready[...], right_w[...], preferred_element_type=jnp.float32
    ).astype(jnp.bfloat16)

    @pl.when(half == 1)
    def _():
        pl.semaphore_wait(barrier, count - 1)
        pl.semaphore_signal(near_sem, inc=1, device_id={"col": twin}, device_id_type=MESH)

    @pl.when(half == 0)
    def _():
        pl.semaphore_wait(near_sem, 1)

    def left_copy(mask):
        return pltpu.make_async_remote_copy(
            src_ref=left_send.at[(half + mask) % 2],
            dst_ref=left_got.at[mask - 1],
            send_sem=lsend_sem.at[mask - 1],
            recv_sem=lgot_sem.at[mask - 1],
            device_id={"col": flip(col, mask, count)},
            device_id_type=MESH,
        )

    right_copy = pltpu.make_async_remote_copy(
        src_ref=right_send,
        dst_ref=right_got,
        send_sem=rsend_sem,
        recv_sem=rgot_sem,
        device_id={"col": twin},
        device_id_type=MESH,
    )
    for mask in range(2, count):
        left_copy(mask).start()
    right_copy.start()
    left_copy(1).start()

    def part_copy(mask, side):
        return pltpu.make_async_remote_copy(
            src_ref=part_send.at[mask, side],
            dst_ref=part_got.at[row, half],
            send_sem=psend_sem.at[mask, side],
            recv_sem=pgot_sem.at[row, half],
            device_id={"row": flip(col, mask, count), "col": twin if side else col},
            device_id_type=MESH,
        )

    def products(mask, side):
        sums = [None] * piece
        for k in range(lines):
            across = right[side, k * width : (k + 1) * width, :]
            for i in range(piece):
                at = k * piece + i
                term = wide[mask, at : at + 1, :] * across
                sums[i] = term if k == 0 else sums[i] + term

        def send():
            for i in range(piece):
                part_send[mask, side, i * width : (i + 1) * width, :] = sums[i].astype(jnp.bfloat16)
            part_copy(mask, side).start()

        if side:
            send()
        else:
            here = flip(col, mask, count) == row

            @pl.when(here)
            def _():
                for i in range(piece):
                    own[i * width : (i + 1) * width, :] = sums[i]

            pl.when(jnp.logical_not(here))(send)

    right[0] = right_send[...].astype(jnp.float32)
    wide[0] = left_send[half].astype(jnp.float32)
    loads[6].wait()
    gate[...] = jax.nn.sigmoid(
        jnp.dot(ready[...], gate_w[...], preferred_element_type=jnp.float32)
    )

    @pl.when(half == 0)
    def _():
        pl.semaphore_wait(barrier, 2 * (count - 1))
        pl.semaphore_signal(far_sem, inc=1, device_id={"col": twin}, device_id_type=MESH)

    @pl.when(half == 1)
    def _():
        pl.semaphore_wait(far_sem, 1)

    products(0, 0)
    right_copy.wait_recv()
    right[1] = right_got[...].astype(jnp.float32)
    products(0, 1)
    for mask in range(1, count):
        left_copy(mask).wait_recv()
        wide[mask] = left_got[mask - 1].astype(jnp.float32)
        products(mask, 0)
        products(mask, 1)
    loads[4].wait()
    loads[5].wait()

    def arrived(peer, part):
        pltpu.make_async_remote_copy(
            src_ref=part_send.at[0, 0],
            dst_ref=part_got.at[peer, part],
            send_sem=psend_sem.at[0, 0],
            recv_sem=pgot_sem.at[peer, part],
            device_id={"row": row, "col": twin},
            device_id_type=MESH,
        ).wait_recv()
        return part_got[peer, part].astype(jnp.float32)

    rows = piece * width
    for part, mixed in ((half, own[...]), (1 - half, arrived(row, 1 - half))):
        for mask in range(1, count):
            mixed = mixed + arrived(flip(row, mask, count), part)
        mixed = (mixed * scale).astype(jnp.bfloat16).astype(jnp.float32)
        scaled = norm_channels(mixed, mid_gain[...]).astype(jnp.bfloat16)
        made = jnp.dot(scaled, out_w[...], preferred_element_type=jnp.float32)
        made = made * gate[pl.ds(pl.multiple_of(part * rows, rows), rows), :]
        result[pl.ds(part * piece, piece)] = made.astype(jnp.bfloat16).reshape(
            piece, width, channels
        )
    for mask in range(1, count):
        left_copy(mask).wait_send()
    right_copy.wait_send()
    for mask in range(count):
        part_copy(mask, 1).wait_send()

        @pl.when(flip(col, mask, count) != row)
        def _(mask=mask):
            part_copy(mask, 0).wait_send()


def fused_body(pair_array, in_gain, left_weight, right_weight, mid_gain, out_weight, out_gate):
    count = lax.axis_size("row")
    lines, width, channels = pair_array.shape
    depth = left_weight.shape[1]
    piece = width // 2
    scale = (lines * count) ** (-0.5)
    low, high = jnp.bfloat16, jnp.float32
    return pl.pallas_call(
        functools.partial(fused, count, scale),
        out_shape=pltpu.VMEM(pair_array.shape, low),
        in_specs=[pl.BlockSpec(memory_space=pl.ANY)] * 7,
        out_specs=pl.BlockSpec(memory_space=pltpu.VMEM),
        scratch_shapes=[
            pltpu.VMEM(pair_array.shape, low),
            pltpu.VMEM((1, channels), high),
            pltpu.VMEM(left_weight.shape, low),
            pltpu.VMEM(right_weight.shape, low),
            pltpu.VMEM((1, depth), high),
            pltpu.VMEM(out_weight.shape, low),
            pltpu.VMEM(out_gate.shape, low),
            pltpu.VMEM((lines * width, channels), low),
            pltpu.VMEM((2, lines * piece, depth), low),
            pltpu.VMEM((count - 1, lines * piece, depth), low),
            pltpu.VMEM((lines * width, depth), low),
            pltpu.VMEM((lines * width, depth), low),
            pltpu.VMEM((2, lines * width, depth), high),
            pltpu.VMEM((count, lines * piece, depth), high),
            pltpu.VMEM((count, 2, piece * width, depth), low),
            pltpu.VMEM((count, 2, piece * width, depth), low),
            pltpu.VMEM((piece * width, depth), high),
            pltpu.VMEM((lines * width, channels), high),
            pltpu.SemaphoreType.DMA((7,)),
            pltpu.SemaphoreType.DMA((count - 1,)),
            pltpu.SemaphoreType.DMA((count - 1,)),
            pltpu.SemaphoreType.DMA,
            pltpu.SemaphoreType.DMA,
            pltpu.SemaphoreType.DMA((count, 2)),
            pltpu.SemaphoreType.DMA((count, 2)),
            pltpu.SemaphoreType.REGULAR,
            pltpu.SemaphoreType.REGULAR,
        ],
        compiler_params=pltpu.CompilerParams(collective_id=0, has_side_effects=True),
        name="triangle",
    )(
        pair_array, in_gain.reshape(1, -1), left_weight, right_weight,
        mid_gain.reshape(1, -1), out_weight, out_gate,
    )


def pick(pair_array, *rest):
    rows, cols = lax.axis_size("row"), lax.axis_size("col")
    square = rows == cols > 1 and rows & (rows - 1) == 0
    square = square and pair_array.shape[0] == pair_array.shape[1]
    square = square and pair_array.shape[1] % 16 == 0
    return (fused_body if square else body)(pair_array, *rest)


def solution(mesh):
    return jax.shard_map(
        pick,
        mesh=mesh,
        in_specs=(
            P(("site", "row"), "col", None),
            P(),
            P("site", None),
            P("site", None),
            P(),
            P("site", None),
            P("site", None),
        ),
        out_specs=P(("site", "row"), "col", None),
        check_vma=False,
    )
```

```python
import functools

import jax
import jax.numpy as jnp
from jax import lax
from jax.experimental import pallas as pl
from jax.experimental.pallas import tpu as pltpu
from jax.sharding import PartitionSpec as P


def norm_channels(values, channel_gain):
    centred = values - jnp.mean(values, axis=-1, keepdims=True)
    return (
        centred
        * lax.rsqrt(jnp.mean(centred * centred, axis=-1, keepdims=True) + 1e-05)
        * channel_gain
    )


def both_factors(pair_in, in_gain, left_weight, right_weight):
    ready = norm_channels(pair_in.astype(jnp.float32), in_gain).astype(jnp.bfloat16)
    ready = lax.optimization_barrier(ready)
    left = jnp.einsum("ijc,cd->ijd", ready, left_weight, preferred_element_type=jnp.float32)
    right = jnp.einsum("ijc,cd->ijd", ready, right_weight, preferred_element_type=jnp.float32)
    return (ready, left.astype(jnp.bfloat16), right.astype(jnp.bfloat16))


def finish_pair(mixed, ready, mid_gain, out_weight, out_gate):
    scaled = norm_channels(mixed.astype(jnp.float32), mid_gain).astype(jnp.bfloat16)
    scaled = lax.optimization_barrier(scaled)
    gate = jax.nn.sigmoid(
        jnp.einsum("ijc,cd->ijd", ready, out_gate, preferred_element_type=jnp.float32)
    )
    return (
        jnp.einsum("ijd,dc->ijc", scaled, out_weight, preferred_element_type=jnp.float32) * gate
    ).astype(jnp.bfloat16)


def body(pair_array, in_gain, left_weight, right_weight, mid_gain, out_weight, out_gate):
    ready, left, right = both_factors(pair_array, in_gain, left_weight, right_weight)
    count = pair_array.shape[0] * lax.axis_size("row")
    left_lines, right_lines = (
        lax.all_to_all(left, "row", split_axis=2, concat_axis=0, tiled=True),
        lax.all_to_all(right, "row", split_axis=2, concat_axis=0, tiled=True),
    )
    strip = jnp.einsum(
        "kid,kjd->ijd",
        lax.all_gather(left_lines, "col", axis=1, tiled=True),
        right_lines,
        preferred_element_type=jnp.float32,
    )
    strip = (strip * count ** (-0.5)).astype(jnp.bfloat16)
    mixed = lax.all_to_all(strip, "row", split_axis=0, concat_axis=2, tiled=True)
    return finish_pair(mixed, ready, mid_gain, out_weight, out_gate)


MESH = pl.DeviceIdType.MESH


def flip(index, mask, count):
    flipped, bit = 0, 1
    while bit < count:
        digit = (index // bit) % 2
        flipped = flipped + bit * ((1 - digit) if mask & bit else digit)
        bit *= 2
    return flipped


def fused(
    count, scale,
    pair_hbm, in_gain_hbm, left_hbm, right_hbm, mid_gain_hbm, out_hbm, gate_hbm,
    result,
    pair, in_gain, left_w, right_w, mid_gain, out_w, gate_w,
    ready, left_send, left_got, right_send, right_got, right, wide, part_send, part_got, own, gate,
    load_sem, lsend_sem, lgot_sem, rsend_sem, rgot_sem, psend_sem, pgot_sem,
    near_sem, far_sem,
):
    row, col = lax.axis_index("row"), lax.axis_index("col")
    half = col % 2
    twin = flip(col, 1, count)
    lines, width = pair.shape[0], pair.shape[1]
    piece = width // 2
    barrier = pltpu.get_barrier_semaphore()
    for n in range(count // 2):
        odd = 2 * n + 1

        @pl.when(odd != col)
        def _(odd=odd):
            pl.semaphore_signal(barrier, inc=1, device_id={"col": odd}, device_id_type=MESH)

    for mask in range(1, count):
        pl.semaphore_signal(
            barrier, inc=1, device_id={"row": flip(row, mask, count), "col": col - half},
            device_id_type=MESH,
        )
    loads = [
        pltpu.make_async_copy(src, dst, load_sem.at[n])
        for n, (src, dst) in enumerate(
            [
                (pair_hbm, pair), (in_gain_hbm, in_gain), (left_hbm, left_w),
                (right_hbm, right_w), (mid_gain_hbm, mid_gain), (out_hbm, out_w),
                (gate_hbm, gate_w),
            ]
        )
    ]
    for load in loads:
        load.start()
    loads[0].wait()
    loads[1].wait()
    channels = pair.shape[2]
    values = pair[...].reshape(lines * width, channels).astype(jnp.float32)
    ready[...] = norm_channels(values, in_gain[...]).astype(jnp.bfloat16)
    loads[2].wait()
    left = jnp.dot(ready[...], left_w[...], preferred_element_type=jnp.float32)
    depth = left.shape[-1]
    left = left.reshape(lines, 2, piece, depth)
    for part in range(2):
        left_send[part] = left[:, part].reshape(lines * piece, depth).astype(jnp.bfloat16)
    loads[3].wait()
    right_send[...] = jnp.dot(
        ready[...], right_w[...], preferred_element_type=jnp.float32
    ).astype(jnp.bfloat16)

    @pl.when(half == 1)
    def _():
        pl.semaphore_wait(barrier, count - 1)
        pl.semaphore_signal(near_sem, inc=1, device_id={"col": twin}, device_id_type=MESH)

    @pl.when(half == 0)
    def _():
        pl.semaphore_wait(near_sem, 1)

    def left_copy(mask):
        return pltpu.make_async_remote_copy(
            src_ref=left_send.at[(half + mask) % 2],
            dst_ref=left_got.at[mask - 1],
            send_sem=lsend_sem.at[mask - 1],
            recv_sem=lgot_sem.at[mask - 1],
            device_id={"col": flip(col, mask, count)},
            device_id_type=MESH,
        )

    right_copy = pltpu.make_async_remote_copy(
        src_ref=right_send,
        dst_ref=right_got,
        send_sem=rsend_sem,
        recv_sem=rgot_sem,
        device_id={"col": twin},
        device_id_type=MESH,
    )
    for mask in range(2, count):
        left_copy(mask).start()
    right_copy.start()
    left_copy(1).start()

    def part_copy(mask, side):
        return pltpu.make_async_remote_copy(
            src_ref=part_send.at[mask, side],
            dst_ref=part_got.at[row, half],
            send_sem=psend_sem.at[mask, side],
            recv_sem=pgot_sem.at[row, half],
            device_id={"row": flip(col, mask, count), "col": twin if side else col},
            device_id_type=MESH,
        )

    def products(mask, side):
        sums = [None] * piece
        for k in range(lines):
            across = right[side, k * width : (k + 1) * width, :]
            for i in range(piece):
                at = k * piece + i
                term = wide[mask, at : at + 1, :] * across
                sums[i] = term if k == 0 else sums[i] + term

        def keep():
            for i in range(piece):
                part_send[mask, side, i * width : (i + 1) * width, :] = sums[i].astype(jnp.bfloat16)

        if side:
            keep()
        else:
            here = flip(col, mask, count) == row

            @pl.when(here)
            def _():
                for i in range(piece):
                    own[i * width : (i + 1) * width, :] = sums[i]

            pl.when(jnp.logical_not(here))(keep)

    def launch(mask, side):
        if side:
            part_copy(mask, side).start()
        else:

            @pl.when(flip(col, mask, count) != row)
            def _():
                part_copy(mask, side).start()

    right[0] = right_send[...].astype(jnp.float32)
    wide[0] = left_send[half].astype(jnp.float32)
    loads[6].wait()
    gate[...] = jax.nn.sigmoid(
        jnp.dot(ready[...], gate_w[...], preferred_element_type=jnp.float32)
    )

    products(0, 0)
    right_copy.wait_recv()
    right[1] = right_got[...].astype(jnp.float32)
    products(0, 1)
    for mask in range(1, count):
        left_copy(mask).wait_recv()
        wide[mask] = left_got[mask - 1].astype(jnp.float32)
        products(mask, 0)
        if mask > 1:
            launch(mask, 0)
        products(mask, 1)
        if mask > 1:
            launch(mask, 1)
        else:
            @pl.when(half == 0)
            def _():
                pl.semaphore_wait(barrier, 2 * (count - 1))
                pl.semaphore_signal(far_sem, inc=1, device_id={"col": twin}, device_id_type=MESH)

            @pl.when(half == 1)
            def _():
                pl.semaphore_wait(far_sem, 1)
            for early in range(2):
                for side in range(2):
                    launch(early, side)
    loads[4].wait()
    loads[5].wait()

    def arrived(peer, part):
        pltpu.make_async_remote_copy(
            src_ref=part_send.at[0, 0],
            dst_ref=part_got.at[peer, part],
            send_sem=psend_sem.at[0, 0],
            recv_sem=pgot_sem.at[peer, part],
            device_id={"row": row, "col": twin},
            device_id_type=MESH,
        ).wait_recv()
        return part_got[peer, part].astype(jnp.float32)

    rows = piece * width
    for part, mixed in ((half, own[...]), (1 - half, arrived(row, 1 - half))):
        for mask in range(1, count):
            mixed = mixed + arrived(flip(row, mask, count), part)
        mixed = (mixed * scale).astype(jnp.bfloat16).astype(jnp.float32)
        scaled = norm_channels(mixed, mid_gain[...]).astype(jnp.bfloat16)
        made = jnp.dot(scaled, out_w[...], preferred_element_type=jnp.float32)
        made = made * gate[pl.ds(pl.multiple_of(part * rows, rows), rows), :]
        result[pl.ds(part * piece, piece)] = made.astype(jnp.bfloat16).reshape(
            piece, width, channels
        )
    for mask in range(1, count):
        left_copy(mask).wait_send()
    right_copy.wait_send()
    for mask in range(count):
        part_copy(mask, 1).wait_send()

        @pl.when(flip(col, mask, count) != row)
        def _(mask=mask):
            part_copy(mask, 0).wait_send()


def fused_body(pair_array, in_gain, left_weight, right_weight, mid_gain, out_weight, out_gate):
    count = lax.axis_size("row")
    lines, width, channels = pair_array.shape
    depth = left_weight.shape[1]
    piece = width // 2
    scale = (lines * count) ** (-0.5)
    low, high = jnp.bfloat16, jnp.float32
    return pl.pallas_call(
        functools.partial(fused, count, scale),
        out_shape=pltpu.VMEM(pair_array.shape, low),
        in_specs=[pl.BlockSpec(memory_space=pl.ANY)] * 7,
        out_specs=pl.BlockSpec(memory_space=pltpu.VMEM),
        scratch_shapes=[
            pltpu.VMEM(pair_array.shape, low),
            pltpu.VMEM((1, channels), high),
            pltpu.VMEM(left_weight.shape, low),
            pltpu.VMEM(right_weight.shape, low),
            pltpu.VMEM((1, depth), high),
            pltpu.VMEM(out_weight.shape, low),
            pltpu.VMEM(out_gate.shape, low),
            pltpu.VMEM((lines * width, channels), low),
            pltpu.VMEM((2, lines * piece, depth), low),
            pltpu.VMEM((count - 1, lines * piece, depth), low),
            pltpu.VMEM((lines * width, depth), low),
            pltpu.VMEM((lines * width, depth), low),
            pltpu.VMEM((2, lines * width, depth), high),
            pltpu.VMEM((count, lines * piece, depth), high),
            pltpu.VMEM((count, 2, piece * width, depth), low),
            pltpu.VMEM((count, 2, piece * width, depth), low),
            pltpu.VMEM((piece * width, depth), high),
            pltpu.VMEM((lines * width, channels), high),
            pltpu.SemaphoreType.DMA((7,)),
            pltpu.SemaphoreType.DMA((count - 1,)),
            pltpu.SemaphoreType.DMA((count - 1,)),
            pltpu.SemaphoreType.DMA,
            pltpu.SemaphoreType.DMA,
            pltpu.SemaphoreType.DMA((count, 2)),
            pltpu.SemaphoreType.DMA((count, 2)),
            pltpu.SemaphoreType.REGULAR,
            pltpu.SemaphoreType.REGULAR,
        ],
        compiler_params=pltpu.CompilerParams(collective_id=0, has_side_effects=True),
        name="triangle",
    )(
        pair_array, in_gain.reshape(1, -1), left_weight, right_weight,
        mid_gain.reshape(1, -1), out_weight, out_gate,
    )


def pick(pair_array, *rest):
    rows, cols = lax.axis_size("row"), lax.axis_size("col")
    square = rows == cols > 1 and rows & (rows - 1) == 0
    square = square and pair_array.shape[0] == pair_array.shape[1]
    square = square and pair_array.shape[1] % 16 == 0
    return (fused_body if square else body)(pair_array, *rest)


def solution(mesh):
    return jax.shard_map(
        pick,
        mesh=mesh,
        in_specs=(
            P(("site", "row"), "col", None),
            P(),
            P("site", None),
            P("site", None),
            P(),
            P("site", None),
            P("site", None),
        ),
        out_specs=P(("site", "row"), "col", None),
        check_vma=False,
    )
```
